32 devices in a mesh: ex: 4 (over z), tp: 4 (over y, x), dp: 2 (over core).
Axes of the slice: x: 2, y: 2, z: 4, core: 2. Of those that a mesh axis runs over, the one named last changes fastest.
Arguments:
- tokens: bfloat16 [1024, 2880], P(('ex', 'dp')), may hold values from -32 to 32
- route_one: int32 [1024, 4], P(('ex', 'dp')), may hold values from 0 to 15, as said below
- route_two: int32 [1024, 4], P(('ex', 'dp')), may hold values from 0 to 15, as said below
- share_one: float32 [1024, 4], P(('ex', 'dp')), may hold values from 0.05 to 0.6
- share_two: float32 [1024, 4], P(('ex', 'dp')), may hold values from 0.05 to 0.6
- gain_one: float32 [2880], replicated, may hold values from 0.5 to 1.5
- gain_two: float32 [2880], replicated, may hold values from 0.5 to 1.5
- gate_up_one: bfloat16 [16, 2880, 2, 2880], P('ex', None, None, 'tp'), may hold values from -0.109375 to 0.109375
- down_one: bfloat16 [16, 2880, 2880], P('ex', 'tp'), may hold values from -0.109375 to 0.109375
- gate_up_two: bfloat16 [16, 2880, 2, 2880], P('ex', None, None, 'tp'), may hold values from -0.109375 to 0.109375
- down_two: bfloat16 [16, 2880, 2880], P('ex', 'tp'), may hold values from -0.109375 to 0.109375
Outputs:
- mixed: bfloat16 [1024, 2880], P(('ex', 'dp'), 'tp')
- load: int32 [2, 16], P(None, 'ex')
The draws below stay inside these ranges and needn't reach their ends.
Inputs may be any that keep to these rules, and one draw needn't show every extreme that they name: `route_one`: each row names 4 different experts; in each aligned block of 128 rows no expert is named by more than 64 rows, and in every block some expert is named by exactly 64 rows. `route_two`: each row names 4 different experts; in each aligned block of 128 rows no expert is named by more than 64 rows, and in every block some expert is named by exactly 64 rows.
All inputs are finite; a program needn't handle non-finite values.
Results may differ from the reference program's by a relative error of at most 0.011.
Values may be sent and summed in bfloat16 or wider, within the bound.
A program may use at most 192 MiB of HBM per device.

```python
import math
import jax
import jax.numpy as jnp
from jax import lax

D = 2880
FF = 2880
TOP = 4
EXPERTS = 16
TOK_DEV = 128
CAP = 64
TOKENS = 1024
N_TP = 4


def draw_tokens(key, part):
    key_rows, key_cols, key_base = jax.random.split(key, 3)
    row_scale = jnp.exp(jax.random.uniform(key_rows, (TOKENS, 1), jnp.float32, math.log(0.5), math.log(2.0)))
    col_scale = jnp.exp(jax.random.uniform(key_cols, (1, D), jnp.float32, math.log(0.4), math.log(4.0)))
    base = jax.random.truncated_normal(key_base, -4.0, 4.0, (TOKENS, D), jnp.float32)
    return (base * row_scale * col_scale).astype(jnp.bfloat16)


def route_table(key):
    blocks = TOKENS // TOK_DEV
    quarter = CAP // 4
    global_order = jax.random.permutation(jax.random.fold_in(key, 7), EXPERTS)
    position = jnp.zeros((EXPERTS,), jnp.int32).at[global_order].set(jnp.arange(EXPERTS, dtype=jnp.int32))
    first_half = position < EXPERTS // 2

    def one_block(block):
        block_key = jax.random.fold_in(key, block + 11)
        key_order, key_rows = jax.random.split(block_key)
        odd = block % 2 == 1
        heavy = jnp.logical_xor(first_half, odd)
        counts = jnp.where(heavy, 3 * quarter, quarter).astype(jnp.int32)
        order = jax.random.permutation(key_order, EXPERTS).astype(jnp.int32)
        heavy_ordered = heavy[order].astype(jnp.int32)
        seen = jnp.cumsum(heavy_ordered)
        adjust = jnp.where((heavy_ordered == 1) & (seen == 1), quarter, 0) - jnp.where((heavy_ordered == 1) & (seen == 2), quarter, 0)
        ordered_counts = counts[order] + adjust.astype(jnp.int32)
        listed = jnp.repeat(order, ordered_counts, total_repeat_length=TOK_DEV * TOP)
        table = listed.reshape(TOP, TOK_DEV).T
        shuffle = jax.random.permutation(key_rows, TOK_DEV)
        return table[shuffle]
    tables = jax.vmap(one_block)(jnp.arange(blocks, dtype=jnp.int32))
    return tables.reshape(TOKENS, TOP).astype(jnp.int32)


def draw_route_one(key, part):
    return route_table(jax.random.fold_in(key, 101))


def draw_route_two(key, part):
    return route_table(jax.random.fold_in(key, 202))


def shard_levels(own_key, extent, cuts, smallest, largest):
    gain, own = 1.0, jax.random.fold_in(own_key, 6)
    for axis_at, shards_of in cuts:
        steps = jnp.exp(jax.random.uniform(jax.random.fold_in(own, axis_at), (shards_of,), jnp.float32, smallest / len(cuts), largest / len(cuts)))
        gain = gain * jnp.repeat(steps, extent[axis_at] // shards_of).reshape([-1 if axis == axis_at else 1 for axis in range(len(extent))])
    return gain


def centred(rng, shape, scale, most, cuts=(), held_as=jnp.bfloat16):
    loudness = shard_levels(rng, shape, cuts, -0.22, 0.18) if cuts else 1.0
    array = jax.random.normal(rng, shape, jnp.float32) * scale * loudness
    return jnp.minimum(jnp.maximum(array, -most), most).astype(held_as)


def setup_inputs(seed: int = 0) -> dict:
    seeds = jax.random.split(jax.random.key(seed), 12)
    return {
        "tokens": draw_tokens(jax.random.fold_in(seeds[11], 71), 0),
        "route_one": draw_route_one(jax.random.fold_in(seeds[11], 71), 0),
        "route_two": draw_route_two(jax.random.fold_in(seeds[11], 71), 0),
        "share_one": jnp.clip(0.05 + 0.55 * jax.random.uniform(seeds[3], (TOKENS, TOP), jnp.float32) ** shard_levels(seeds[3], (TOKENS, TOP), ((0, 8),), -0.2, 0.2), 0.05, 0.6),
        "share_two": jnp.clip(0.05 + 0.55 * jax.random.uniform(seeds[4], (TOKENS, TOP), jnp.float32) ** shard_levels(seeds[4], (TOKENS, TOP), ((0, 8),), -0.2, 0.2), 0.05, 0.6),
        "gain_one": jnp.clip(1.0 + 0.1 * jax.random.normal(seeds[5], (D,), jnp.float32), 0.5, 1.5),
        "gain_two": jnp.clip(1.0 + 0.1 * jax.random.normal(seeds[6], (D,), jnp.float32), 0.5, 1.5),
        "gate_up_one": centred(seeds[7], (EXPERTS, D, 2, FF), D ** -0.5, 0.109375, ((0, 4), (3, 4))),
        "down_one": centred(seeds[8], (EXPERTS, FF, D), FF ** -0.5, 0.109375, ((0, 4), (1, 4))),
        "gate_up_two": centred(seeds[9], (EXPERTS, D, 2, FF), D ** -0.5, 0.109375, ((0, 4), (3, 4))),
        "down_two": centred(seeds[10], (EXPERTS, FF, D), FF ** -0.5, 0.109375, ((0, 4), (1, 4))),
    }


norm_eps = 1e-05
glu_alpha = 1.702

def expert_layer(stream, routes, shares, gains, gate_up, down_proj):
    tokens_all = stream.shape[0]
    model_width = stream.shape[1]
    experts = gate_up.shape[0]
    hidden_width = gate_up.shape[3]
    top_count = routes.shape[1]
    blocks = tokens_all // TOK_DEV
    share_width = hidden_width // N_TP
    values = stream.astype(jnp.float32)
    inverse = lax.rsqrt(lax.optimization_barrier(jnp.mean(values * values, axis=1, keepdims=True)) + norm_eps)
    normed = (values * inverse * gains[None, :]).astype(jnp.bfloat16)
    flattened = routes.reshape(blocks, TOK_DEV * top_count)
    matches = (flattened[:, :, None] == jnp.arange(experts, dtype=jnp.int32)[None, None, :]).astype(jnp.int32)
    slot_rank = jnp.cumsum(matches, axis=1) - 1
    slot_index = lax.optimization_barrier(jnp.sum(slot_rank * matches, axis=2))
    target = (flattened * CAP + slot_index).astype(jnp.int32)
    block_index = jnp.broadcast_to(jnp.arange(blocks, dtype=jnp.int32)[:, None], target.shape)
    repeated = jnp.repeat(normed.reshape(blocks, TOK_DEV, model_width), top_count, axis=1)
    packed = jnp.zeros((blocks, experts * CAP, model_width), jnp.bfloat16).at[block_index, target].set(repeated)
    per_expert = packed.reshape(blocks, experts, CAP, model_width).transpose(1, 0, 2, 3).reshape(experts, blocks * CAP, model_width)

    def one_expert(operands):
        inputs, weight_in, weight_down = operands
        hidden = jnp.dot(inputs.astype(jnp.float32), weight_in.reshape(model_width, 2 * hidden_width).astype(jnp.float32), precision=lax.Precision.HIGHEST)
        gate_part = hidden[:, :hidden_width]
        up_part = hidden[:, hidden_width:]
        activated = (gate_part * jax.nn.sigmoid(glu_alpha * gate_part) * (up_part + 1.0)).astype(jnp.bfloat16)
        summed = jnp.zeros((inputs.shape[0], model_width), jnp.float32)
        for section in range(N_TP):
            lower = section * share_width
            upper = lower + share_width
            portion = jnp.dot(activated[:, lower:upper].astype(jnp.float32), weight_down[lower:upper].astype(jnp.float32), precision=lax.Precision.HIGHEST)
            rounded = lax.optimization_barrier(portion.astype(jnp.bfloat16))
            summed = summed + rounded.astype(jnp.float32)
        return summed.astype(jnp.bfloat16)
    outputs = lax.map(one_expert, (per_expert, gate_up, down_proj))
    returned = outputs.reshape(experts, blocks, CAP, model_width).transpose(1, 0, 2, 3).reshape(blocks, experts * CAP, model_width)
    picked = returned[block_index, target].astype(jnp.float32).reshape(tokens_all, top_count, model_width)
    mixed = values + lax.optimization_barrier(jnp.sum(shares[:, :, None] * picked, axis=1))
    counted = lax.optimization_barrier(jnp.sum(matches, axis=(0, 1))).astype(jnp.int32)
    return (mixed.astype(jnp.bfloat16), counted)

def reference(tokens, route_one, route_two, share_one, share_two, gain_one, gain_two, gate_up_one, down_one, gate_up_two, down_two):
    stream, load_first = expert_layer(tokens, route_one, share_one, gain_one, gate_up_one, down_one)
    mixed, load_second = expert_layer(stream, route_two, share_two, gain_two, gate_up_two, down_two)
    return (mixed, jnp.stack([load_first, load_second]))
```

```python
import functools

import jax
import jax.numpy as jnp
from jax import lax
from jax.experimental import pallas as pl
from jax.experimental.pallas import tpu as pltpu
from jax.sharding import PartitionSpec as P

norm_eps = 1e-05
glu_alpha = 1.702


def placement(routes, experts, capacity):
    tokens_here, top_count = routes.shape
    flattened = routes.reshape(tokens_here * top_count)
    matches = (flattened[:, None] == jnp.arange(experts, dtype=jnp.int32)[None, :]).astype(
        jnp.int32
    )
    slot_rank = jnp.cumsum(matches, axis=0) - 1
    slot_index = jnp.sum(slot_rank * matches, axis=1)
    target = (flattened * capacity + slot_index).reshape(tokens_here, top_count)
    return target


def choosers(target, shares, local_count, capacity, group):
    sources, top_count, tokens_here = target.shape
    groups = sources // group
    wide = group * capacity
    first = lax.axis_index("ex") * (local_count * capacity)
    local = target.astype(jnp.int32) - first
    inside = (local >= 0) & (local < local_count * capacity)
    place = (jnp.arange(sources, dtype=jnp.int32) % group)[:, None, None]
    column = (local // capacity) * wide + place * capacity + local % capacity
    column = jnp.where(inside, column, -1)
    column = column.reshape(groups, group, top_count, tokens_here)
    column = column.transpose(0, 1, 3, 2).reshape(groups, group * tokens_here, top_count)
    share = shares.reshape(groups, group, top_count, tokens_here)
    share = share.transpose(0, 1, 3, 2).reshape(groups, group * tokens_here, top_count)
    slots = jnp.arange(local_count * wide, dtype=jnp.int32)
    equal = column[:, :, :, None] == slots
    chooser = jnp.any(equal, axis=2).astype(jnp.bfloat16)
    weight = jnp.sum(jnp.where(equal, share[:, :, :, None], 0.0), axis=(1, 2))
    weight = weight.reshape(groups, local_count, wide).transpose(1, 0, 2)
    return chooser, weight.reshape(local_count, 1, groups * wide)


def expert_kernel(group, x_ref, gain_ref, choose_ref, weight_ref, up_ref, down_ref, y_ref,
                  packed, outs):
    step = pl.program_id(0)
    steps = pl.num_programs(0)
    sources, width, tokens_here = x_ref.shape
    groups = sources // group
    wide = packed.shape[1] // groups
    share_width = down_ref.shape[1]

    @pl.when(step == 0)
    def _():
        for s in range(sources):
            values = x_ref[s].astype(jnp.float32)
            inverse = lax.rsqrt(jnp.mean(values * values, axis=0, keepdims=True) + norm_eps)
            y_ref[s] = (values * inverse * gain_ref[...]).astype(jnp.bfloat16)

    at = pl.multiple_of(step * wide, wide)
    for g in range(groups):
        normed = [y_ref[g * group + s] for s in range(group)]
        normed = jnp.concatenate(normed, axis=1)
        packed[:, g * wide:(g + 1) * wide] = jnp.dot(
            normed, choose_ref[g, :, pl.ds(at, wide)], preferred_element_type=jnp.float32
        ).astype(jnp.bfloat16)
    gate = jnp.dot(up_ref[0, :share_width], packed[...], preferred_element_type=jnp.float32)
    up = jnp.dot(up_ref[0, share_width:], packed[...], preferred_element_type=jnp.float32)
    act = gate * jax.nn.sigmoid(glu_alpha * gate) * (up + 1.0) * weight_ref[0]
    act = act.T.astype(jnp.bfloat16)
    out = jnp.dot(act, down_ref[0], preferred_element_type=jnp.float32).astype(jnp.bfloat16)
    for g in range(groups):
        outs[g, pl.ds(at, wide)] = out[g * wide:(g + 1) * wide]

    @pl.when(step == steps - 1)
    def _():
        for g in range(groups):
            mixed = jnp.dot(choose_ref[g], outs[g], preferred_element_type=jnp.float32)
            mixed = mixed.astype(jnp.bfloat16).T
            for s in range(group):
                y_ref[g * group + s] = mixed[:, s * tokens_here:(s + 1) * tokens_here]


def experts_here(x, gains, chooser, weight, gate_up, down_proj, group):
    sources, width, tokens_here = x.shape
    local_count, _, share_width = gate_up.shape[0], gate_up.shape[2], gate_up.shape[3]
    groups = sources // group
    slots = weight.shape[2]
    wide = slots // groups
    rows_in = gate_up.transpose(0, 2, 3, 1).reshape(local_count, 2 * share_width, width)
    whole = lambda shape: pl.BlockSpec(shape, lambda e: (0,) * len(shape))
    return pl.pallas_call(
        functools.partial(expert_kernel, group),
        grid=(local_count,),
        out_shape=jax.ShapeDtypeStruct((sources, width, tokens_here), jnp.bfloat16),
        in_specs=[
            whole(x.shape),
            whole((width, 1)),
            whole(chooser.shape),
            pl.BlockSpec((1, 1, slots), lambda e: (e, 0, 0)),
            pl.BlockSpec((1, 2 * share_width, width), lambda e: (e, 0, 0)),
            pl.BlockSpec((1, share_width, width), lambda e: (e, 0, 0)),
        ],
        out_specs=whole(x.shape),
        scratch_shapes=[
            pltpu.VMEM((width, slots), jnp.bfloat16),
            pltpu.VMEM((groups, local_count * wide, width), jnp.bfloat16),
        ],
        compiler_params=pltpu.CompilerParams(
            dimension_semantics=("arbitrary",), vmem_limit_bytes=60 * 1024 * 1024
        ),
        cost_estimate=pl.CostEstimate(
            flops=6 * local_count * slots * width * share_width,
            bytes_accessed=6 * local_count * width * share_width,
            transcendentals=0,
        ),
        name="experts_here",
    )(x, gains[:, None], chooser, weight, rows_in, down_proj)


MESH = pl.DeviceIdType.MESH


def greet(with_dp=False):
    barrier = pltpu.get_barrier_semaphore()
    total = 0
    for axis in ("ex", "tp"):
        count = lax.axis_size(axis)
        for ahead in range(1, count):
            peer = lax.rem(lax.axis_index(axis) + ahead, count)
            pl.semaphore_signal(barrier, inc=1, device_id={axis: peer}, device_id_type=MESH)
            total += 1
    if with_dp:
        for peer in dp_peers():
            pl.semaphore_signal(barrier, inc=1, device_id=peer, device_id_type=MESH)
            total += 1
    pl.semaphore_wait(barrier, total)


def dp_peers():
    ex_count, dp_count = lax.axis_size("ex"), lax.axis_size("dp")
    return [
        {
            "ex": lax.rem(lax.axis_index("ex") + ahead, ex_count),
            "dp": lax.rem(lax.axis_index("dp") + across, dp_count),
        }
        for across in range(1, dp_count)
        for ahead in range(ex_count)
    ]


def gather_small_kernel(own_ref, small_ref, all_ref, smalls_ref, send_ex, recv_ex, send_tp,
                        recv_tp, send_small, recv_small):
    ex, dp = lax.axis_index("ex"), lax.axis_index("dp")
    ex_count = lax.axis_size("ex")
    greet(True)
    peers = [
        {"ex": lax.rem(ex + ahead, ex_count), "dp": dp} for ahead in range(1, ex_count)
    ] + dp_peers()
    copies = []
    for at, peer in enumerate(peers):
        copy = pltpu.make_async_remote_copy(
            src_ref=small_ref,
            dst_ref=smalls_ref.at[dp, ex],
            send_sem=send_small.at[at],
            recv_sem=recv_small.at[at],
            device_id=peer,
            device_id_type=MESH,
        )
        copy.start()
        copies.append(copy)
    smalls_ref[dp, ex] = small_ref[...]
    gather_steps(own_ref, all_ref, send_ex, recv_ex, send_tp, recv_tp)
    for copy in copies:
        copy.wait_recv()
    for copy in copies:
        copy.wait_send()


def gather_kernel(own_ref, all_ref, send_ex, recv_ex, send_tp, recv_tp):
    greet()
    gather_steps(own_ref, all_ref, send_ex, recv_ex, send_tp, recv_tp)


def gather_steps(own_ref, all_ref, send_ex, recv_ex, send_tp, recv_tp):
    ex_count, tp_count = all_ref.shape[:2]
    ex, tp = lax.axis_index("ex"), lax.axis_index("tp")
    started = []

    def push(source, block, axis, index, count, ahead, send, recv):
        copy = pltpu.make_async_remote_copy(
            src_ref=source,
            dst_ref=all_ref.at[block, tp],
            send_sem=send,
            recv_sem=recv,
            device_id={axis: lax.rem(index + ahead, count)},
            device_id_type=MESH,
        )
        copy.start()
        return copy

    along = {}
    for ahead in range(1, ex_count):
        along[ahead] = push(
            own_ref, ex, "ex", ex, ex_count, ahead, send_ex.at[ahead], recv_ex.at[ahead]
        )
    for ahead in range(1, tp_count):
        started.append(push(
            own_ref, ex, "tp", tp, tp_count, ahead, send_tp.at[0, ahead], recv_tp.at[0, ahead]
        ))
    all_ref[ex, tp] = own_ref[...]
    for back in range(1, ex_count):
        along[back].wait_recv()
        block = lax.rem(ex + ex_count - back, ex_count)
        for ahead in range(1, tp_count):
            started.append(push(
                all_ref.at[block, tp], block, "tp", tp, tp_count, ahead,
                send_tp.at[back, ahead], recv_tp.at[back, ahead],
            ))
    for copy in started:
        copy.wait_recv()
    for copy in started:
        copy.wait_send()
    for copy in along.values():
        copy.wait_send()


def gather_all(own, small=None):
    ex_count, tp_count = lax.axis_size("ex"), lax.axis_size("tp")
    rows, lanes = own.shape
    if small is not None:
        dp_count = lax.axis_size("dp")
        gathered, smalls = pl.pallas_call(
            gather_small_kernel,
            out_shape=(
                jax.ShapeDtypeStruct((ex_count, tp_count, rows, lanes), own.dtype),
                jax.ShapeDtypeStruct((dp_count, ex_count) + small.shape, small.dtype),
            ),
            in_specs=[pl.BlockSpec(memory_space=pltpu.VMEM)] * 2,
            out_specs=[pl.BlockSpec(memory_space=pltpu.VMEM)] * 2,
            scratch_shapes=[
                pltpu.SemaphoreType.DMA((ex_count,)),
                pltpu.SemaphoreType.DMA((ex_count,)),
                pltpu.SemaphoreType.DMA((ex_count, tp_count)),
                pltpu.SemaphoreType.DMA((ex_count, tp_count)),
                pltpu.SemaphoreType.DMA((ex_count * dp_count,)),
                pltpu.SemaphoreType.DMA((ex_count * dp_count,)),
            ],
            compiler_params=pltpu.CompilerParams(collective_id=2, has_side_effects=True),
            name="gather_small",
        )(own, small)
        return gathered.reshape(ex_count, tp_count * rows, lanes), smalls
    gathered = pl.pallas_call(
        gather_kernel,
        out_shape=jax.ShapeDtypeStruct((ex_count, tp_count, rows, lanes), own.dtype),
        in_specs=[pl.BlockSpec(memory_space=pltpu.VMEM)],
        out_specs=pl.BlockSpec(memory_space=pltpu.VMEM),
        scratch_shapes=[
            pltpu.SemaphoreType.DMA((ex_count,)),
            pltpu.SemaphoreType.DMA((ex_count,)),
            pltpu.SemaphoreType.DMA((ex_count, tp_count)),
            pltpu.SemaphoreType.DMA((ex_count, tp_count)),
        ],
        compiler_params=pltpu.CompilerParams(collective_id=0, has_side_effects=True),
        name="gather_all",
    )(own)
    return gathered.reshape(ex_count, tp_count * rows, lanes)


def scatter_kernel(part_ref, base_ref, out_ref, from_tp, sums, from_ex,
                   send_tp, recv_tp, send_ex, recv_ex):
    ex_count, tp_count = part_ref.shape[:2]
    ex, tp = lax.axis_index("ex"), lax.axis_index("tp")
    greet()
    order = list(range(1, ex_count)) + [0]
    across = {}
    for back in order:
        block = lax.rem(ex + back, ex_count)
        for ahead in range(1, tp_count):
            peer = lax.rem(tp + ahead, tp_count)
            copy = pltpu.make_async_remote_copy(
                src_ref=part_ref.at[block, peer],
                dst_ref=from_tp.at[back, ahead - 1],
                send_sem=send_tp.at[back, ahead],
                recv_sem=recv_tp.at[back, ahead],
                device_id={"tp": peer},
                device_id_type=MESH,
            )
            copy.start()
            across[back, ahead] = copy
    along = {}
    for back in order:
        block = lax.rem(ex + back, ex_count)
        total = part_ref[block, tp].astype(jnp.float32)
        for ahead in range(1, tp_count):
            across[back, ahead].wait_recv()
            total = total + from_tp[back, ahead - 1].astype(jnp.float32)
        if back == 0:
            out_ref[...] = base_ref[...].astype(jnp.float32) + total
            continue
        sums[back] = total.astype(jnp.bfloat16)
        along[back] = pltpu.make_async_remote_copy(
            src_ref=sums.at[back],
            dst_ref=from_ex.at[back],
            send_sem=send_ex.at[back],
            recv_sem=recv_ex.at[back],
            device_id={"ex": block},
            device_id_type=MESH,
        )
        along[back].start()
    for copy in along.values():
        copy.wait_recv()
    total = out_ref[...]
    for back in along:
        total = total + from_ex[back].astype(jnp.float32)
    out_ref[...] = total
    for copy in across.values():
        copy.wait_send()
    for copy in along.values():
        copy.wait_send()


def scatter_sum(partial, base):
    ex_count, tp_count = lax.axis_size("ex"), lax.axis_size("tp")
    rows, lanes = base.shape
    total = pl.pallas_call(
        scatter_kernel,
        out_shape=jax.ShapeDtypeStruct((rows, lanes), jnp.float32),
        in_specs=[pl.BlockSpec(memory_space=pltpu.VMEM)] * 2,
        out_specs=pl.BlockSpec(memory_space=pltpu.VMEM),
        scratch_shapes=[
            pltpu.VMEM((ex_count, tp_count - 1, rows, lanes), jnp.bfloat16),
            pltpu.VMEM((ex_count, rows, lanes), jnp.bfloat16),
            pltpu.VMEM((ex_count, rows, lanes), jnp.bfloat16),
            pltpu.SemaphoreType.DMA((ex_count, tp_count)),
            pltpu.SemaphoreType.DMA((ex_count, tp_count)),
            pltpu.SemaphoreType.DMA((ex_count,)),
            pltpu.SemaphoreType.DMA((ex_count,)),
        ],
        compiler_params=pltpu.CompilerParams(collective_id=1, has_side_effects=True),
        name="scatter_sum",
    )(partial.reshape(ex_count, tp_count, rows, lanes), base)
    return total.astype(jnp.bfloat16)


def body(
    tokens,
    route_one,
    route_two,
    share_one,
    share_two,
    gain_one,
    gain_two,
    gate_up_one,
    down_one,
    gate_up_two,
    down_two,
):
    ex_count = lax.axis_size("ex")
    tp_count = lax.axis_size("tp")
    tokens_here, width = tokens.shape
    top_count = route_one.shape[1]
    local_count = gate_up_one.shape[0]
    experts = local_count * ex_count
    capacity = 2 * tokens_here * top_count // experts
    capacity = min(tokens_here, capacity)
    group = 2 if ex_count % 2 == 0 else 1
    col_share = width // tp_count
    columns = tokens.T
    own = lax.dynamic_slice_in_dim(columns, lax.axis_index("tp") * col_share, col_share, 0)

    target_one = placement(route_one, experts, capacity)
    target_two = placement(route_two, experts, capacity)
    small = jnp.concatenate(
        [target_one.T.astype(jnp.float32), target_two.T.astype(jnp.float32), share_one.T, share_two.T]
    )
    gathered, smalls = gather_all(own, small)
    smalls = smalls.reshape(-1, ex_count, 4, top_count, tokens_here)
    chosen = smalls[:, :, :2].astype(jnp.int32) // capacity
    mine = lax.axis_index("ex") * local_count + jnp.arange(local_count, dtype=jnp.int32)
    load = jnp.sum((chosen[..., None] == mine).astype(jnp.int32), axis=(0, 1, 3, 4))
    small = lax.dynamic_index_in_dim(smalls, lax.axis_index("dp"), 0, keepdims=False)
    choose_one, weight_one = choosers(small[:, 0], small[:, 2], local_count, capacity, group)
    choose_two, weight_two = choosers(small[:, 1], small[:, 3], local_count, capacity, group)

    first = experts_here(gathered, gain_one, choose_one, weight_one, gate_up_one, down_one, group)
    stream = scatter_sum(first, own)
    again = gather_all(stream)
    second = experts_here(again, gain_two, choose_two, weight_two, gate_up_two, down_two, group)
    mixed = scatter_sum(second, stream)
    return (mixed.T, load)


def solution(mesh):
    in_specs = (
        P(("ex", "dp"), None),
        P(("ex", "dp"), None),
        P(("ex", "dp"), None),
        P(("ex", "dp"), None),
        P(("ex", "dp"), None),
        P(),
        P(),
        P("ex", None, None, "tp"),
        P("ex", "tp", None),
        P("ex", None, None, "tp"),
        P("ex", "tp", None),
    )
    out_specs = (P(("ex", "dp"), "tp"), P(None, "ex"))
    return jax.shard_map(body, mesh=mesh, in_specs=in_specs, out_specs=out_specs, check_vma=False)
```
